32 devices in a mesh: dp: 16 (over z, x, core), tensor: 2 (over y).
Axes of the slice: x: 2, y: 2, z: 4, core: 2. Of those that a mesh axis runs over, the one named last changes fastest.
Arguments:
- hidden_in: bfloat16 [4096, 1152], P('dp'), may hold values from -6 to 6
- condition: bfloat16 [112, 1152], P('dp'), may hold values from -6 to 6
- heights: int32 [16, 7], P('dp'), may hold values from 3 to 6, as said below
- widths: int32 [16, 7], P('dp'), may hold values from 3 to 6, as said below
- ada_weight: bfloat16 [1152, 6912], P('dp', 'tensor'), may hold values from -0.1875 to 0.1875
- attn_weight: bfloat16 [1152, 4, 1152], P('dp', None, 'tensor'), may hold values from -0.1875 to 0.1875
- forget_weight: bfloat16 [1152, 16], P('dp', 'tensor'), may hold values from -0.1875 to 0.1875
- forget_bias: float32 [16], P('tensor'), may hold values from -4 to 3
- conv_weight: bfloat16 [9, 1152], P(None, 'tensor'), may hold values from -1.796875 to 1.796875
- out_weight: bfloat16 [1152, 1152], P('tensor', 'dp'), may hold values from -0.1875 to 0.1875
- up_weight: bfloat16 [1152, 4608], P('dp', 'tensor'), may hold values from -0.1875 to 0.1875
- down_weight: bfloat16 [4608, 1152], P('tensor', 'dp'), may hold values from -0.09375 to 0.09375
- cotangent: bfloat16 [4096, 1152], P('dp'), may hold values from -6 to 6
Outputs:
- hidden_out: bfloat16 [4096, 1152], P('dp')
- grad_hidden: bfloat16 [4096, 1152], P('dp')
- grad_condition: bfloat16 [112, 1152], P('dp')
- grad_ada: float32 [1152, 6912], P('dp', 'tensor')
- grad_attn: float32 [1152, 4, 1152], P('dp', None, 'tensor')
- grad_forget: float32 [1152, 16], P('dp', 'tensor')
- grad_bias: float32 [16], P('tensor')
- grad_conv: float32 [9, 1152], P(None, 'tensor')
- grad_out_weight: float32 [1152, 1152], P('tensor', 'dp')
- grad_up: float32 [1152, 4608], P('dp', 'tensor')
- grad_down: float32 [4608, 1152], P('tensor', 'dp')
The draws below stay inside these ranges and needn't reach their ends.
Inputs may be any that keep to these rules, and one draw needn't show every extreme that they name: `heights`: each packed sequence holds 7 images laid back to back from its first slot; the slots after them are empty. `widths`: as for heights.
All inputs are finite; a program needn't handle non-finite values.
Results may differ from the reference program's by a relative error of at most 0.011.
Values may be sent and summed in bfloat16 or wider, within the bound.
A program may use at most 256 MiB of HBM per device.

```python
import jax
import jax.numpy as jnp
from jax import lax

D = 1152
HEADS = 16
FF = 4608
BLOCK = 64
MAXSIDE = 6
IMGS = 7
LEN = 256
SEQ_DEV = 1
SEQS = 16
TOKENS = 4096
IMAGES = 112


def draw_sides(key, salt_value):
    side_values = jax.random.randint(jax.random.fold_in(key, salt_value), (SEQS, IMGS), 3, MAXSIDE + 1, dtype=jnp.int32)
    flat_index = jnp.arange(SEQS * IMGS, dtype=jnp.int32).reshape(SEQS, IMGS)
    side_values = jnp.where(flat_index == 0, MAXSIDE, side_values)
    return jnp.where(flat_index == 1, 3, side_values).astype(jnp.int32)


def draw_heights(key, part):
    return draw_sides(key, 11)


def draw_widths(key, part):
    return draw_sides(key, 23)


def block_levels(rng, shape, shards, smallest, largest):
    def one(axis_at, shards_of):
        steps = jax.random.uniform(jax.random.fold_in(jax.random.fold_in(rng, 6), axis_at), (shards_of,), jnp.float32, smallest / len(shards), largest / len(shards))
        return jnp.repeat(jnp.exp(steps), shape[axis_at] // shards_of).reshape((-1,) + (1,) * (len(shape) - axis_at - 1))

    gain = one(*shards[0])
    for cut in shards[1:]:
        gain = gain * one(*cut)
    return gain


def gaussian(own_key, extent, scale, limit, pieces=(), kind=jnp.bfloat16):
    values = jax.random.normal(own_key, extent, jnp.float32) * scale
    if len(pieces) > 0:
        values = block_levels(own_key, extent, pieces, -0.22, 0.18) * values
    return jnp.clip(values, min=-limit, max=limit).astype(kind)


def setup_inputs(seed: int = 0) -> dict:
    arg_keys = jax.random.split(jax.random.key(seed), 14)
    return {
        "hidden_in": gaussian(arg_keys[0], (TOKENS, D), 1.0, 6.0, ((0, 16),)),
        "condition": gaussian(arg_keys[1], (IMAGES, D), 1.0, 6.0, ((0, 16),)),
        "heights": draw_heights(jax.random.fold_in(arg_keys[13], 71), 0),
        "widths": draw_widths(jax.random.fold_in(arg_keys[13], 71), 0),
        "ada_weight": gaussian(arg_keys[4], (D, 6 * D), D ** -0.5, 0.1875, ((0, 16), (1, 2))),
        "attn_weight": gaussian(arg_keys[5], (D, 4, D), D ** -0.5, 0.1875, ((0, 16), (2, 2))),
        "forget_weight": gaussian(arg_keys[6], (D, HEADS), D ** -0.5, 0.1875, ((0, 16), (1, 2))),
        "forget_bias": jnp.clip(-4.0 + 7.0 * jax.random.uniform(arg_keys[7], (HEADS,), jnp.float32) ** block_levels(arg_keys[7], (HEADS,), ((0, 2),), -0.2, 0.2), -4.0, 3.0),
        "conv_weight": gaussian(arg_keys[8], (9, D), 0.3, 1.796875, ((1, 2),)),
        "out_weight": gaussian(arg_keys[9], (D, D), D ** -0.5, 0.1875, ((0, 2), (1, 16))),
        "up_weight": gaussian(arg_keys[10], (D, FF), D ** -0.5, 0.1875, ((0, 16), (1, 2))),
        "down_weight": gaussian(arg_keys[11], (FF, D), FF ** -0.5, 0.09375, ((0, 2), (1, 16))),
        "cotangent": gaussian(arg_keys[12], (TOKENS, D), 1.0, 6.0, ((0, 16),)),
    }


gate_norm = 16.0
norm_epsilon = 1e-06
head_epsilon = 1e-05
highest_precision = lax.Precision.HIGHEST

@jax.custom_vjp
def low(v):
    return lax.optimization_barrier(v.astype(jnp.bfloat16)).astype(jnp.float32)

@jax.custom_vjp
def low_back(v):
    return v

def low_keep(v):
    return (low(v), None)

def low_pass(kept, grad):
    return (grad,)

def back_keep(v):
    return (v, None)

def back_low(kept, grad):
    return (low(grad),)
low.defvjp(low_keep, low_pass)
low_back.defvjp(back_keep, back_low)

def layout(heights, widths, length):
    sequence_count, number_of_images = heights.shape
    image_area = (heights * widths).astype(jnp.int32)
    image_ends = jnp.cumsum(image_area, axis=1).astype(jnp.int32)
    starts = (image_ends - image_area).astype(jnp.int32)
    position = jnp.arange(length, dtype=jnp.int32)
    segment = lax.optimization_barrier(jnp.sum((position[None, :, None] >= image_ends[:, None, :]).astype(jnp.int32), axis=2)).astype(jnp.int32)
    choose_rows = segment[:, :, None] == jnp.arange(number_of_images, dtype=jnp.int32)[None, None, :]
    zero_int = jnp.zeros((), jnp.int32)
    start_at = lax.optimization_barrier(jnp.sum(jnp.where(choose_rows, starts[:, None, :], zero_int), axis=2)).astype(jnp.int32)
    image_width = jnp.maximum(lax.optimization_barrier(jnp.sum(jnp.where(choose_rows, widths[:, None, :], zero_int), axis=2)).astype(jnp.int32), 1)
    image_height = lax.optimization_barrier(jnp.sum(jnp.where(choose_rows, heights[:, None, :], zero_int), axis=2)).astype(jnp.int32)
    offset_in = position[None, :] - start_at
    row_index = offset_in // image_width
    col_index = offset_in - row_index * image_width
    is_valid = segment < number_of_images
    seq_base = jnp.arange(sequence_count, dtype=jnp.int32)[:, None]
    token_keys = (segment + seq_base * (number_of_images + 1)).reshape(-1).astype(jnp.int32)
    tap_list = []
    for vertical in (-1, 0, 1):
        for lateral in (-1, 0, 1):
            inside = is_valid & (row_index + vertical >= 0) & (row_index + vertical < image_height) & (col_index + lateral >= 0) & (col_index + lateral < image_width)
            target = jnp.clip(position[None, :] + vertical * image_width + lateral, 0, length - 1) + seq_base * length
            tap_list.append((target.reshape(-1).astype(jnp.int32), inside.reshape(-1).astype(jnp.float32)))
    return (choose_rows.astype(jnp.float32), token_keys, tap_list)

def modulate(values, shift, scale):
    centre = values - lax.optimization_barrier(jnp.mean(values, axis=1, keepdims=True))
    spread = lax.optimization_barrier(jnp.mean(centre * centre, axis=1, keepdims=True))
    return centre * lax.rsqrt(spread + norm_epsilon) * (1.0 + scale) + shift

def gelu_tanh(values):
    return jax.nn.gelu(values, approximate=True)

def token_mixer(queries, keys_in, values, gate_raw, forget_raw, conv_kernel, token_keys, tap_list):
    number_of_tokens, channels = queries.shape
    head_count = forget_raw.shape[1]
    head_size = channels // head_count
    block_count = number_of_tokens // BLOCK
    log_decay = jax.nn.log_sigmoid(forget_raw) / gate_norm
    cumulative = jnp.cumsum(log_decay.reshape(block_count, BLOCK, head_count), axis=1)
    decay_rows = jnp.transpose(cumulative, (0, 2, 1))
    query_blocks = (jax.nn.elu(queries) + 1.0).reshape(block_count, BLOCK, head_count, head_size)
    key_blocks = (jax.nn.elu(keys_in) + 1.0).reshape(block_count, BLOCK, head_count, head_size)
    value_blocks = values.reshape(block_count, BLOCK, head_count, head_size)
    block_keys = token_keys.reshape(block_count, BLOCK)
    position = jnp.arange(BLOCK, dtype=jnp.int32)
    lower = position[:, None] >= position[None, :]
    same_heads = ((block_keys[:, :, None] == block_keys[:, None, :]) & lower[None, :, :])[:, None, :, :]
    exponent = decay_rows[:, :, :, None] - decay_rows[:, :, None, :]
    decays = jnp.where(same_heads, jnp.exp(jnp.where(same_heads, exponent, 0.0)), 0.0)
    scores = jnp.einsum('bthk,bshk->bhts', query_blocks, key_blocks, precision=highest_precision)
    inside_part = jnp.einsum('bhts,bshk->bthk', scores * decays, value_blocks, precision=highest_precision)
    last_decay = decay_rows[:, :, -1]
    last_key = block_keys[:, -1]
    member = (block_keys == last_key[:, None]).astype(jnp.float32)
    end_weight = member[:, :, None] * jnp.exp(last_decay[:, None, :] - cumulative)
    weighted = key_blocks * end_weight[:, :, :, None]
    summary = jnp.einsum('bshk,bshj->bhkj', weighted, value_blocks, precision=highest_precision)
    prior_key = jnp.concatenate([jnp.full((1,), -1, jnp.int32), last_key[:-1]])
    keep_state = (last_key == prior_key).astype(jnp.float32)
    factor = keep_state[:, None] * jnp.exp(last_decay)

    def advance(carry_state, inputs):
        scale_now, added = inputs
        return (scale_now[:, None, None] * carry_state + added, carry_state)
    initial = jnp.zeros((head_count, head_size, head_size), jnp.float32)
    final_state, start_states = lax.scan(advance, initial, (factor, summary))
    carries = (block_keys == prior_key[:, None]).astype(jnp.float32)
    lifted = query_blocks * jnp.exp(cumulative)[:, :, :, None] * carries[:, :, None, None]
    carried_part = jnp.einsum('bthk,bhkj->bthj', lifted, start_states, precision=highest_precision)
    attended = (inside_part + carried_part).reshape(number_of_tokens, head_count, head_size)
    normed = attended * lax.rsqrt(lax.optimization_barrier(jnp.mean(attended * attended, axis=2, keepdims=True)) + head_epsilon)
    gated_out = normed.reshape(number_of_tokens, channels) * jax.nn.silu(gate_raw)
    spatial = jnp.zeros_like(gated_out)
    for tap_number, (target, inside) in enumerate(tap_list):
        spatial = spatial + conv_kernel[tap_number][None, :] * jnp.take(gated_out, target, axis=0) * inside[:, None]
    return gated_out + spatial

def forward(hidden, cond_group, weight_args, choose_rows, token_keys, tap_list):
    ada_weight, attn_weight, forget_weight, forget_bias, conv_weight, out_weight, up_weight, down_weight = weight_args
    sequence_count, length, number_of_images = choose_rows.shape
    number_of_tokens, hidden_width = hidden.shape
    act_cond = low(jax.nn.silu(cond_group))
    modulation_vectors = low_back(jnp.dot(act_cond, ada_weight, precision=highest_precision))
    token_wise = jnp.einsum('jyq,jqu->jyu', choose_rows, modulation_vectors.reshape(sequence_count, number_of_images, 6 * hidden_width), precision=highest_precision).reshape(number_of_tokens, 6 * hidden_width)
    shift_one, scale_one, gate_one, shift_two, scale_two, gate_two = jnp.split(token_wise, 6, axis=1)
    xm_one = low(modulate(hidden, shift_one, scale_one))
    projected = jnp.dot(xm_one, attn_weight.reshape(hidden_width, 4 * hidden_width), precision=highest_precision).reshape(number_of_tokens, 4, hidden_width)
    queries = low(low_back(projected[:, 0]))
    keys_low = low(low_back(projected[:, 1]))
    values = low(low_back(projected[:, 2]))
    gate_raw = low_back(projected[:, 3])
    forget_raw = jnp.dot(xm_one, forget_weight, precision=highest_precision) + forget_bias
    mixed_out = low(token_mixer(queries, keys_low, values, gate_raw, forget_raw, conv_weight, token_keys, tap_list))
    attn_out = low_back(jnp.dot(mixed_out, out_weight, precision=highest_precision))
    after_attn = hidden + gate_one * attn_out
    xm_two = low(modulate(after_attn, shift_two, scale_two))
    up_value = low_back(jnp.dot(xm_two, up_weight, precision=highest_precision))
    act_value = low(gelu_tanh(up_value))
    down_value = low_back(jnp.dot(act_value, down_weight, precision=highest_precision))
    return after_attn + gate_two * down_value

def reference(hidden_in, condition, heights, widths, ada_weight, attn_weight, forget_weight, forget_bias, conv_weight, out_weight, up_weight, down_weight, cotangent):
    group_seqs = SEQ_DEV * 8
    group_count = SEQS // group_seqs
    group_tokens = group_seqs * LEN
    weights = tuple((weight_item.astype(jnp.float32) for weight_item in (ada_weight, attn_weight, forget_weight, forget_bias, conv_weight, out_weight, up_weight, down_weight)))
    hidden_groups = hidden_in.astype(jnp.float32).reshape(group_count, group_tokens, D)
    cond_groups = condition.astype(jnp.float32).reshape(group_count, group_seqs * IMGS, D)
    height_groups = heights.reshape(group_count, group_seqs, IMGS)
    width_groups = widths.reshape(group_count, group_seqs, IMGS)
    upstream_groups = cotangent.astype(jnp.float32).reshape(group_count, group_tokens, D)

    def one_group(totals, inputs):
        hidden, cond_group, group_heights, group_widths, upstream = inputs
        choose_rows, token_keys, tap_list = layout(group_heights, group_widths, LEN)

        def whole_layer(hidden_arg, cond_arg, *weight_args):
            return forward(hidden_arg, cond_arg, weight_args, choose_rows, token_keys, tap_list)
        result, pullback = jax.vjp(whole_layer, hidden, cond_group, *weights)
        gradients = pullback(upstream)
        totals = tuple((running + gradient for running, gradient in zip(totals, gradients[2:])))
        return (totals, (result.astype(jnp.bfloat16), gradients[0].astype(jnp.bfloat16), gradients[1].astype(jnp.bfloat16)))
    initial = tuple((jnp.zeros_like(weight_item) for weight_item in weights))
    totals, stacked = lax.scan(one_group, initial, (hidden_groups, cond_groups, height_groups, width_groups, upstream_groups))
    out_groups, grad_groups, cond_grads = stacked
    grad_ada, grad_attn, grad_forget, grad_bias, grad_conv, grad_out_weight, grad_up, grad_down = totals
    return (out_groups.reshape(TOKENS, D), grad_groups.reshape(TOKENS, D), cond_grads.reshape(IMAGES, D), grad_ada, grad_attn, grad_forget, grad_bias, grad_conv, grad_out_weight, grad_up, grad_down)
```

```python
import functools

import jax
import jax.numpy as jnp
import numpy as np
from jax import lax
from jax.sharding import PartitionSpec as P

BLOCK = 64


gate_norm = 16.0
norm_epsilon = 1e-06
head_epsilon = 1e-05
highest_precision = lax.Precision.HIGHEST


def layout(heights, widths, length):
    sequence_count, number_of_images = heights.shape
    image_area = heights * widths
    image_ends = jnp.cumsum(image_area, axis=1)
    starts = image_ends - image_area
    position = jnp.arange(length, dtype=jnp.int32)
    segment = jnp.sum((position[None, :, None] >= image_ends[:, None, :]).astype(jnp.int32), axis=2)
    choose_rows = (
        segment[:, :, None] == jnp.arange(number_of_images, dtype=jnp.int32)[None, None, :]
    )
    zero_int = jnp.zeros((), jnp.int32)
    start_at = jnp.sum(jnp.where(choose_rows, starts[:, None, :], zero_int), axis=2)
    image_width = jnp.maximum(
        jnp.sum(jnp.where(choose_rows, widths[:, None, :], zero_int), axis=2), 1
    )
    image_height = jnp.sum(jnp.where(choose_rows, heights[:, None, :], zero_int), axis=2)
    offset_in = position[None, :] - start_at
    row_index = offset_in // image_width
    col_index = offset_in - row_index * image_width
    is_valid = segment < number_of_images
    seq_base = jnp.arange(sequence_count, dtype=jnp.int32)[:, None]
    token_keys = (segment + seq_base * (number_of_images + 1)).reshape(-1)
    tap_list = []
    for vertical in (-1, 0, 1):
        for lateral in (-1, 0, 1):
            inside = (
                is_valid
                & (row_index + vertical >= 0)
                & (row_index + vertical < image_height)
                & (col_index + lateral >= 0)
                & (col_index + lateral < image_width)
            )
            target = (
                jnp.clip(position[None, :] + vertical * image_width + lateral, 0, length - 1)
                + seq_base * length
            )
            tap_list.append((target.reshape(-1), inside.reshape(-1).astype(jnp.float32)))
    return (choose_rows.astype(jnp.float32), token_keys, tap_list)


def modulate(values, shift, scale):
    centre = values - jnp.mean(values, axis=1, keepdims=True)
    spread = jnp.mean(centre * centre, axis=1, keepdims=True)
    return centre * lax.rsqrt(spread + norm_epsilon) * (1.0 + scale) + shift


def gelu_tanh(values):
    return jax.nn.gelu(values, approximate=True)


def phase_masks(ranks):
    if ranks == 16:
        return ((4, 8), (2,), (1,))
    return tuple((1 << bit,) for bit in reversed(range(ranks.bit_length() - 1)))


def offsets_of(group):
    found = []
    for choice in range(1 << len(group)):
        mask = 0
        for place, bit in enumerate(group):
            if choice >> place & 1:
                mask ^= bit
        found.append(mask)
    return found


def relative_owners(ranks):
    owners = [0]
    for group in phase_masks(ranks):
        owners = [mask ^ owner for mask in offsets_of(group) for owner in owners]
    return owners


def swap(value, mask, ranks):
    return lax.ppermute(value, "dp", [(i, i ^ mask) for i in range(ranks)])


def gather_pieces(piece, ranks, split):
    pieces = [piece[None]]
    for group in phase_masks(ranks):
        if not split or ranks != 16 or group == (1,):
            pieces = [jnp.concatenate(pieces, axis=0)] if len(pieces) > 1 else pieces
        pieces = [
            (swap(item, mask, ranks) if mask else item)
            for mask in offsets_of(group)
            for item in pieces
        ]
    return jnp.concatenate(pieces, axis=0)


def scatter_sum(partial, ranks, wire):
    current = partial.astype(wire)
    groups = phase_masks(ranks)
    for place in reversed(range(len(groups))):
        offsets = offsets_of(groups[place])
        size = current.shape[0] // len(offsets)
        total = current[:size].astype(jnp.float32)
        for choice, mask in enumerate(offsets):
            if mask:
                part = swap(current[choice * size : (choice + 1) * size], mask, ranks)
                total = total + part.astype(jnp.float32)
        current = total.astype(wire) if place else total
    return current[0]


def exchange_pieces(pieces, ranks):
    groups = phase_masks(ranks)
    sizes = [len(offsets_of(group)) for group in groups]
    trailing = pieces.shape[1:]
    current = pieces.reshape(tuple(reversed(sizes)) + trailing)
    for place, group in enumerate(groups):
        axis = len(groups) - 1 - place
        parts = []
        for choice, mask in enumerate(offsets_of(group)):
            part = lax.slice_in_dim(current, choice, choice + 1, axis=axis)
            parts.append(swap(part, mask, ranks) if mask else part)
        current = jnp.concatenate(parts, axis=axis)
    return current.reshape((ranks,) + trailing)


def sum_everywhere(value, ranks):
    for group in reversed(phase_masks(ranks)):
        for bit in group:
            value = value + swap(value, bit, ranks)
    return value


def other_side(value):
    return lax.ppermute(value, "tensor", [(0, 1), (1, 0)])


def tensor_total(partial_terms):
    mine = partial_terms.astype(jnp.bfloat16)
    theirs = other_side(mine)
    return mine.astype(jnp.float32) + theirs.astype(jnp.float32)


def dot_rows(left, right):
    return lax.dot_general(
        left, right, (((1,), (1,)), ((), ())), preferred_element_type=jnp.float32
    )


def dot_tokens(left, right):
    return lax.dot_general(
        left, right, (((0,), (0,)), ((), ())), preferred_element_type=jnp.float32
    ).astype(jnp.bfloat16)


def token_mixer(queries, keys_in, values, gate_raw, forget_raw, conv_kernel, token_keys, tap_list):
    number_of_tokens, channels = queries.shape
    head_count = forget_raw.shape[1]
    head_size = channels // head_count
    block_count = number_of_tokens // BLOCK
    log_decay = jax.nn.log_sigmoid(forget_raw) / gate_norm
    cumulative = jnp.cumsum(log_decay.reshape(block_count, BLOCK, head_count), axis=1)
    decay_rows = jnp.transpose(cumulative, (0, 2, 1))
    query_blocks = (jax.nn.elu(queries) + 1.0).reshape(block_count, BLOCK, head_count, head_size)
    key_blocks = (jax.nn.elu(keys_in) + 1.0).reshape(block_count, BLOCK, head_count, head_size)
    value_blocks = values.reshape(block_count, BLOCK, head_count, head_size)
    block_keys = token_keys.reshape(block_count, BLOCK)
    position = jnp.arange(BLOCK, dtype=jnp.int32)
    lower = position[:, None] >= position[None, :]
    same_heads = ((block_keys[:, :, None] == block_keys[:, None, :]) & lower[None, :, :])[
        :, None, :, :
    ]
    exponent = decay_rows[:, :, :, None] - decay_rows[:, :, None, :]
    decays = jnp.where(same_heads, jnp.exp(jnp.where(same_heads, exponent, 0.0)), 0.0)
    scores = jnp.einsum("bthk,bshk->bhts", query_blocks, key_blocks, precision=highest_precision)
    inside_part = jnp.einsum(
        "bhts,bshk->bthk", scores * decays, value_blocks, precision=highest_precision
    )
    last_decay = decay_rows[:, :, -1]
    last_key = block_keys[:, -1]
    member = (block_keys == last_key[:, None]).astype(jnp.float32)
    end_weight = member[:, :, None] * jnp.exp(last_decay[:, None, :] - cumulative)
    weighted = key_blocks * end_weight[:, :, :, None]
    summary = jnp.einsum("bshk,bshj->bhkj", weighted, value_blocks, precision=highest_precision)
    prior_key = jnp.concatenate([jnp.full((1,), -1, jnp.int32), last_key[:-1]])
    keep_state = (last_key == prior_key).astype(jnp.float32)
    factor = keep_state[:, None] * jnp.exp(last_decay)

    def advance(carry_state, inputs):
        scale_now, added = inputs
        return (scale_now[:, None, None] * carry_state + added, carry_state)

    initial = jnp.zeros((head_count, head_size, head_size), jnp.float32)
    final_state, start_states = lax.scan(advance, initial, (factor, summary))
    carries = (block_keys == prior_key[:, None]).astype(jnp.float32)
    lifted = query_blocks * jnp.exp(cumulative)[:, :, :, None] * carries[:, :, None, None]
    carried_part = jnp.einsum("bthk,bhkj->bthj", lifted, start_states, precision=highest_precision)
    attended = (inside_part + carried_part).reshape(number_of_tokens, head_count, head_size)
    normed = attended * lax.rsqrt(
        jnp.mean(attended * attended, axis=2, keepdims=True) + head_epsilon
    )
    gated_out = normed.reshape(number_of_tokens, channels) * jax.nn.silu(gate_raw)
    spatial = jnp.zeros_like(gated_out)
    for tap_number, (target, inside) in enumerate(tap_list):
        spatial = (
            spatial
            + conv_kernel[tap_number][None, :]
            * jnp.take(gated_out, target, axis=0)
            * inside[:, None]
        )
    return gated_out + spatial


def body(
    hidden_in,
    condition,
    heights,
    widths,
    ada_weight,
    attn_weight,
    forget_weight,
    forget_bias,
    conv_weight,
    out_weight,
    up_weight,
    down_weight,
    cotangent,
    ranks=1,
):
    low = jnp.bfloat16
    sequence_count, number_of_images = heights.shape
    number_of_tokens, hidden_width = hidden_in.shape
    length = number_of_tokens // sequence_count
    half_width = conv_weight.shape[1]
    images_here = condition.shape[0]
    rows = up_weight.shape[0]
    me = lax.axis_index("dp")
    side = lax.axis_index("tensor")
    choose_rows, token_keys, tap_list = layout(heights, widths, length)

    owners = np.repeat(np.array(relative_owners(ranks), np.int32), rows)
    natural = (me ^ owners) * rows + np.tile(np.arange(rows, dtype=np.int32), ranks)
    order = (jnp.arange(hidden_width, dtype=jnp.int32)[:, None] == natural[None, :]).astype(low)

    def to_relative(value):
        return jnp.dot(value, order, preferred_element_type=jnp.float32)

    def to_natural(value):
        return dot_rows(value, order)

    head_count = forget_weight.shape[1]
    proj_width = 4 * half_width + head_count
    shard_attn = jnp.concatenate([attn_weight.reshape(rows, 4 * half_width), forget_weight], axis=1)
    full_attn = gather_pieces(shard_attn, ranks, True).reshape(hidden_width, proj_width)

    cond_all = gather_pieces(condition, ranks, False).reshape(ranks * images_here, hidden_width)
    cond_own = jnp.dot(cond_all, order[:, :rows], preferred_element_type=jnp.float32)
    act_own = jax.nn.silu(cond_own).astype(low)
    mod_partial = jnp.dot(act_own, ada_weight, preferred_element_type=jnp.float32)
    mod_half = scatter_sum(mod_partial.reshape(ranks, images_here, -1), ranks, jnp.float32)
    mod_other = other_side(mod_half)
    mod_first = jnp.where(side == 0, mod_half, mod_other).reshape(images_here * 3, hidden_width)
    mod_second = jnp.where(side == 0, mod_other, mod_half).reshape(images_here * 3, hidden_width)
    mod_rel = jnp.dot(
        jnp.concatenate([mod_first, mod_second], axis=0),
        order.astype(jnp.float32),
        precision=highest_precision,
    ).reshape(2, sequence_count, number_of_images, 3, hidden_width)

    token_wise = jnp.einsum(
        "jyq,hjqcu->hcjyu", choose_rows, mod_rel, precision=highest_precision
    ).reshape(6, number_of_tokens, hidden_width)
    shift_one, scale_one, gate_one, shift_two, scale_two, gate_two = (
        token_wise[0],
        token_wise[1],
        token_wise[2],
        token_wise[3],
        token_wise[4],
        token_wise[5],
    )
    full_out = gather_pieces(out_weight.T, ranks, True).reshape(hidden_width, half_width)
    full_up = gather_pieces(up_weight, ranks, True).reshape(hidden_width, -1)
    full_down = gather_pieces(down_weight.T, ranks, True).reshape(hidden_width, -1)

    hidden_float = to_relative(hidden_in)
    upstream = to_relative(cotangent)
    modulated_one, norm_one_back = jax.vjp(modulate, hidden_float, shift_one, scale_one)
    xm_one = modulated_one.astype(low)
    projected = jnp.dot(xm_one, full_attn, preferred_element_type=jnp.float32)
    queries = projected[:, :half_width].astype(low)
    keys_low = projected[:, half_width : 2 * half_width].astype(low)
    values = projected[:, 2 * half_width : 3 * half_width].astype(low)
    gate_raw = projected[:, 3 * half_width : 4 * half_width]
    forget_raw = projected[:, 4 * half_width :] + forget_bias
    mixer_local = functools.partial(token_mixer, token_keys=token_keys, tap_list=tap_list)
    mixed_out, mixer_back = jax.vjp(
        mixer_local,
        queries.astype(jnp.float32),
        keys_low.astype(jnp.float32),
        values.astype(jnp.float32),
        gate_raw,
        forget_raw,
        conv_weight.astype(jnp.float32),
    )
    mixed_low = mixed_out.astype(low)
    attn_out = tensor_total(dot_rows(mixed_low, full_out))
    after_attn = hidden_float + gate_one * attn_out
    modulated_two, norm_two_back = jax.vjp(modulate, after_attn, shift_two, scale_two)
    xm_two = modulated_two.astype(low)
    up_value = jnp.dot(xm_two, full_up, preferred_element_type=jnp.float32)
    act_value, gelu_back = jax.vjp(gelu_tanh, up_value)
    act_ffn = act_value.astype(low)
    down_value = tensor_total(dot_rows(act_ffn, full_down))
    hidden_out = to_natural((after_attn + gate_two * down_value).astype(low)).astype(low)

    delta_down = (gate_two * upstream).astype(low)
    delta_gate_two = upstream * down_value
    delta_act = jnp.dot(delta_down, full_down, preferred_element_type=jnp.float32)
    grad_down = scatter_sum(dot_tokens(delta_down, act_ffn).reshape(ranks, rows, -1), ranks, low)
    delta_up = gelu_back(delta_act)[0].astype(low)
    grad_up = scatter_sum(dot_tokens(xm_two, delta_up).reshape(ranks, rows, -1), ranks, low)
    delta_xm_two = tensor_total(dot_rows(delta_up, full_up))
    delta_after, delta_shift_two, delta_scale_two = norm_two_back(delta_xm_two)
    delta_after = delta_after + upstream
    delta_attn = (gate_one * delta_after).astype(low)
    delta_gate_one = delta_after * attn_out
    grad_out = scatter_sum(dot_tokens(delta_attn, mixed_low).reshape(ranks, rows, -1), ranks, low)
    delta_mixed = jnp.dot(delta_attn, full_out, preferred_element_type=jnp.float32)
    delta_query, delta_key, delta_value, delta_gate, delta_forget, delta_conv = mixer_back(
        delta_mixed
    )
    delta_proj = jnp.concatenate(
        [delta_query, delta_key, delta_value, delta_gate, delta_forget], axis=1
    ).astype(low)
    small = jnp.concatenate(
        [delta_conv, jnp.pad(jnp.sum(delta_forget, axis=0)[None], ((0, 0), (0, half_width - head_count)))],
        axis=0,
    )
    small = sum_everywhere(small, ranks)
    grad_conv, grad_bias = small[:-1], small[-1, :head_count]
    grad_proj = scatter_sum(dot_tokens(xm_one, delta_proj).reshape(ranks, rows, -1), ranks, low)
    delta_xm_one = tensor_total(dot_rows(delta_proj, full_attn))
    delta_input, delta_shift_one, delta_scale_one = norm_one_back(delta_xm_one)
    grad_hidden = to_natural((delta_after + delta_input).astype(low)).astype(low)
    first_group = jnp.stack([delta_shift_one, delta_scale_one, delta_gate_one], axis=0)
    second_group = jnp.stack([delta_shift_two, delta_scale_two, delta_gate_two], axis=0)
    delta_tokens = jnp.where(side == 0, first_group, second_group)
    delta_mod = jnp.einsum(
        "mxz,cmxk->mzck",
        choose_rows,
        delta_tokens.reshape(3, sequence_count, length, hidden_width),
        precision=highest_precision,
    ).reshape(images_here * 3, hidden_width)
    delta_mod = to_natural(delta_mod.astype(low)).astype(low).reshape(images_here, -1)
    delta_all = gather_pieces(delta_mod, ranks, False).reshape(ranks * images_here, -1)
    grad_ada = lax.dot_general(
        act_own, delta_all, (((0,), (0,)), ((), ())), preferred_element_type=jnp.float32
    )
    delta_cond = dot_rows(delta_all, ada_weight)
    delta_cond = delta_cond + other_side(delta_cond)
    delta_cond = exchange_pieces(delta_cond.reshape(ranks, images_here, rows), ranks)
    delta_cond = jnp.transpose(delta_cond, (1, 0, 2)).reshape(images_here, hidden_width)
    delta_cond = lax.dot_general(
        delta_cond,
        order.astype(jnp.float32),
        (((1,), (1,)), ((), ())),
        precision=highest_precision,
    )
    _, silu_back = jax.vjp(jax.nn.silu, condition.astype(jnp.float32))
    grad_condition = silu_back(delta_cond)[0].astype(low)
    return (
        hidden_out,
        grad_hidden,
        grad_condition,
        grad_ada,
        grad_proj[:, : 4 * half_width].reshape(rows, 4, half_width),
        grad_proj[:, 4 * half_width :],
        grad_bias,
        grad_conv,
        grad_out.T,
        grad_up,
        grad_down.T,
    )


def solution(mesh):
    in_specs = (
        P("dp", None),
        P("dp", None),
        P("dp", None),
        P("dp", None),
        P("dp", "tensor"),
        P("dp", None, "tensor"),
        P("dp", "tensor"),
        P("tensor"),
        P(None, "tensor"),
        P("tensor", "dp"),
        P("dp", "tensor"),
        P("tensor", "dp"),
        P("dp", None),
    )
    out_specs = (
        P("dp", None),
        P("dp", None),
        P("dp", None),
        P("dp", "tensor"),
        P("dp", None, "tensor"),
        P("dp", "tensor"),
        P("tensor"),
        P(None, "tensor"),
        P("tensor", "dp"),
        P("dp", "tensor"),
        P("tensor", "dp"),
    )
    return jax.shard_map(functools.partial(body, ranks=mesh.shape["dp"]), mesh=mesh, in_specs=in_specs, out_specs=out_specs, check_vma=False)
```

```python
import functools

import jax
import jax.numpy as jnp
import numpy as np
from jax import lax
from jax.experimental import pallas as pl
from jax.experimental.pallas import tpu as pltpu
from jax.sharding import PartitionSpec as P

gate_norm = 16.0
norm_epsilon = 1e-06
head_epsilon = 1e-05
highest_precision = lax.Precision.HIGHEST


def modulate(values, shift, scale):
    centre = values - jnp.mean(values, axis=1, keepdims=True)
    spread = jnp.mean(centre * centre, axis=1, keepdims=True)
    return centre * lax.rsqrt(spread + norm_epsilon) * (1.0 + scale) + shift


def gelu_tanh(values):
    return jax.nn.gelu(values, approximate=True)


def phase_masks(ranks):
    if ranks == 16:
        return ((4, 8), (2,), (1,))
    return tuple((1 << bit,) for bit in reversed(range(ranks.bit_length() - 1)))


def offsets_of(group):
    found = []
    for choice in range(1 << len(group)):
        mask = 0
        for place, bit in enumerate(group):
            if choice >> place & 1:
                mask ^= bit
        found.append(mask)
    return found


def relative_owners(ranks):
    owners = [0]
    for group in phase_masks(ranks):
        owners = [mask ^ owner for mask in offsets_of(group) for owner in owners]
    return owners


def swap(value, mask, ranks):
    return lax.ppermute(value, "dp", [(i, i ^ mask) for i in range(ranks)])


def gather_pieces(piece, ranks, split):
    pieces = [piece[None]]
    for group in phase_masks(ranks):
        if not split or ranks != 16 or group == (1,):
            pieces = [jnp.concatenate(pieces, axis=0)] if len(pieces) > 1 else pieces
        pieces = [
            (swap(item, mask, ranks) if mask else item)
            for mask in offsets_of(group)
            for item in pieces
        ]
    return jnp.concatenate(pieces, axis=0)


def scatter_sum(partial, ranks, wire):
    current = partial.astype(wire)
    groups = phase_masks(ranks)
    for place in reversed(range(len(groups))):
        offsets = offsets_of(groups[place])
        size = current.shape[0] // len(offsets)
        total = current[:size].astype(jnp.float32)
        for choice, mask in enumerate(offsets):
            if mask:
                part = swap(current[choice * size : (choice + 1) * size], mask, ranks)
                total = total + part.astype(jnp.float32)
        current = total.astype(wire) if place else total
    return current[0]


def exchange_pieces(pieces, ranks):
    groups = phase_masks(ranks)
    sizes = [len(offsets_of(group)) for group in groups]
    trailing = pieces.shape[1:]
    current = pieces.reshape(tuple(reversed(sizes)) + trailing)
    for place, group in enumerate(groups):
        axis = len(groups) - 1 - place
        parts = []
        for choice, mask in enumerate(offsets_of(group)):
            part = lax.slice_in_dim(current, choice, choice + 1, axis=axis)
            parts.append(swap(part, mask, ranks) if mask else part)
        current = jnp.concatenate(parts, axis=axis)
    return current.reshape((ranks,) + trailing)


def sum_everywhere(value, ranks):
    for group in reversed(phase_masks(ranks)):
        for bit in group:
            value = value + swap(value, bit, ranks)
    return value


def other_side(value):
    return lax.ppermute(value, "tensor", [(0, 1), (1, 0)])


def tensor_total(partial_terms):
    mine = partial_terms.astype(jnp.bfloat16)
    theirs = other_side(mine)
    return mine.astype(jnp.float32) + theirs.astype(jnp.float32)


def dot_rows(left, right):
    return lax.dot_general(
        left, right, (((1,), (1,)), ((), ())), preferred_element_type=jnp.float32
    )


def dot_tokens(left, right):
    return lax.dot_general(
        left, right, (((0,), (0,)), ((), ())), preferred_element_type=jnp.float32
    ).astype(jnp.bfloat16)


def positions(ends, sides, length):
    heights, widths = sides
    slot = lax.broadcasted_iota(jnp.int32, (length, 1), 0)
    along = lax.broadcasted_iota(jnp.int32, (1, length), 1)
    group = jnp.zeros((length, 1), jnp.int32)
    group_row = jnp.zeros((1, length), jnp.int32)
    for end in ends:
        group = group + (slot >= end).astype(jnp.int32)
        group_row = group_row + (along >= end).astype(jnp.int32)
    start = jnp.zeros((length, 1), jnp.int32)
    high = jnp.zeros((length, 1), jnp.int32)
    wide = jnp.zeros((length, 1), jnp.int32)
    for index, end in enumerate(ends):
        here = group == index
        area = heights[index] * widths[index]
        start = jnp.where(here, end - area, start)
        high = jnp.where(here, heights[index], high)
        wide = jnp.where(here, widths[index], wide)
    offset = (slot - start).astype(jnp.float32)
    span = jnp.maximum(wide, 1)
    row = jnp.floor((offset + 0.5) / span.astype(jnp.float32)).astype(jnp.int32)
    col = slot - start - row * span
    return slot, group, group_row, row, col, high, wide


def read_sides(heights_ref, widths_ref):
    count = heights_ref.shape[1]
    heights = [heights_ref[0, i] for i in range(count)]
    widths = [widths_ref[0, i] for i in range(count)]
    ends, total = [], 0
    for high, wide in zip(heights, widths):
        total = total + high * wide
        ends.append(total)
    return ends, (heights, widths)


def tap_matrix(tap, place, images, length):
    slot, group, _, row, col, high, wide = place
    down = tap // 3 - 1
    right = tap - (down + 1) * 3 - 1
    inside = (
        (group < images)
        & (row + down >= 0)
        & (row + down < high)
        & (col + right >= 0)
        & (col + right < wide)
    )
    target = jnp.where(inside, slot + down * wide + right, -1)
    along = lax.broadcasted_iota(jnp.int32, (length, length), 1)
    return jnp.where(along == target, 1.0, 0.0).astype(jnp.bfloat16)


def feature_map(value):
    return jnp.where(value > 0, value + 1.0, jnp.exp(jnp.minimum(value, 0.0)))


def decay_sums(forget, length):
    log_decay = (jnp.minimum(forget, 0.0) - jnp.log1p(jnp.exp(-jnp.abs(forget)))) / gate_norm
    down = lax.broadcasted_iota(jnp.int32, (length, length), 0)
    along = lax.broadcasted_iota(jnp.int32, (length, length), 1)
    lower = jnp.where(along <= down, 1.0, 0.0)
    return jnp.dot(
        lower, log_decay, precision=highest_precision, preferred_element_type=jnp.float32
    )


def head_masks(pair, head_size, width):
    lane = lax.broadcasted_iota(jnp.int32, (1, width), 1)
    low = pair * (2 * head_size - 128)
    return (
        (lane >= low) & (lane < low + head_size),
        (lane >= low + head_size) & (lane < low + 2 * head_size),
    )


def pick_column(table, index):
    lane = lax.broadcasted_iota(jnp.int32, table.shape, 1)
    return jnp.sum(jnp.where(lane == index, table, 0.0), axis=1, keepdims=True)


def by_head(masks, first, second):
    return jnp.where(masks[0], first, jnp.where(masks[1], second, 0.0))


def pair_weights(pair, cum_ref, cum_t_ref, group, group_row, length):
    down = lax.broadcasted_iota(jnp.int32, (length, length), 0)
    along = lax.broadcasted_iota(jnp.int32, (length, length), 1)
    same = (group == group_row) & (down >= along)
    cum = cum_ref[...]
    weights = []
    for which in range(2):
        head = 2 * pair + which
        exponent = pick_column(cum, head) - cum_t_ref[pl.ds(head, 1), :]
        weights.append(jnp.where(same, jnp.exp(jnp.where(same, exponent, 0.0)), 0.0))
    return jnp.concatenate(weights, axis=0)


def contract_rows(left, right):
    return lax.dot_general(
        left, right, (((0,), (0,)), ((), ())), preferred_element_type=jnp.float32
    )


def mixer_forward(
    heads,
    heights_ref,
    widths_ref,
    proj_ref,
    bias_ref,
    taps_ref,
    mixed_ref,
    attended_ref,
    q_ref,
    k_ref,
    v_ref,
    a_ref,
    cum_ref,
    cum_t_ref,
):
    low = jnp.bfloat16
    length = proj_ref.shape[0]
    width = mixed_ref.shape[1]
    head_size = width // heads
    images = heights_ref.shape[1]
    place = positions(*read_sides(heights_ref, widths_ref), length)
    for ref in (q_ref, k_ref, v_ref, a_ref):
        ref[...] = jnp.zeros_like(ref)
    for index, ref in enumerate((q_ref, k_ref)):
        value = proj_ref[:, index * width : (index + 1) * width].astype(low).astype(jnp.float32)
        ref[:, :width] = feature_map(value).astype(low)
    v_ref[:, :width] = proj_ref[:, 2 * width : 3 * width].astype(low)
    forget = proj_ref[:, 4 * width : 4 * width + heads] + bias_ref[...]
    cum_ref[...] = jnp.zeros_like(cum_ref)
    cum_ref[:, :heads] = decay_sums(forget, length)
    cum_t_ref[...] = jnp.transpose(cum_ref[...])

    def one_pair(pair, _):
        window = pl.ds(pl.multiple_of(pair * 128, 128), 256)
        masks = head_masks(pair, head_size, 256)
        query = q_ref[:, window]
        zero = jnp.zeros_like(query)
        stacked = jnp.concatenate(
            [jnp.where(masks[0], query, zero), jnp.where(masks[1], query, zero)], axis=0
        )
        scores = dot_rows(stacked, k_ref[:, window])
        weights = pair_weights(pair, cum_ref, cum_t_ref, place[1], place[2], length)
        found = jnp.dot(
            (scores * weights).astype(low), v_ref[:, window], preferred_element_type=jnp.float32
        )
        a_ref[:, window] += by_head(masks, found[:length], found[length:])
        return 0

    lax.fori_loop(0, heads // 2, one_pair, 0)
    attended_ref[...] = a_ref[:, :width]

    def normalise(pair, _):
        window = pl.ds(pl.multiple_of(pair * 128, 128), 256)
        masks = head_masks(pair, head_size, 256)
        value = a_ref[:, window]
        square = value * value
        roots = [
            lax.rsqrt(
                jnp.sum(jnp.where(mask, square, 0.0), axis=1, keepdims=True) / head_size
                + head_epsilon
            )
            for mask in masks
        ]
        a_ref[:, window] = value * jnp.where(
            masks[0], roots[0], jnp.where(masks[1], roots[1], 1.0)
        )
        return 0

    lax.fori_loop(0, heads // 2, normalise, 0)
    gate = proj_ref[:, 3 * width : 4 * width]
    gated = a_ref[:, :width] * (gate * jax.nn.sigmoid(gate))
    a_ref[:, :width] = gated
    gated_low = gated.astype(low)

    def one_tap(tap, _):
        matrix = tap_matrix(tap, place, images, length)
        found = jnp.dot(matrix, gated_low, preferred_element_type=jnp.float32)
        a_ref[:, :width] += taps_ref[pl.ds(tap, 1), :] * found
        return 0

    lax.fori_loop(0, 9, one_tap, 0)
    mixed_ref[...] = a_ref[:, :width].astype(low)


def mixer_backward(
    heads,
    heights_ref,
    widths_ref,
    proj_ref,
    bias_ref,
    taps_ref,
    attended_ref,
    mixed_grad_ref,
    proj_grad_ref,
    taps_grad_ref,
    bias_grad_ref,
    q_ref,
    k_ref,
    v_ref,
    o_ref,
    n_ref,
    u_ref,
    dq_ref,
    dk_ref,
    dv_ref,
    cum_ref,
    cum_t_ref,
    decay_ref,
):
    low = jnp.bfloat16
    length = proj_ref.shape[0]
    width = attended_ref.shape[1]
    head_size = width // heads
    images = heights_ref.shape[1]
    place = positions(*read_sides(heights_ref, widths_ref), length)
    for ref in (q_ref, k_ref, v_ref, o_ref, n_ref, u_ref, dq_ref, dk_ref, dv_ref, decay_ref):
        ref[...] = jnp.zeros_like(ref)
    for index, ref in enumerate((q_ref, k_ref)):
        value = proj_ref[:, index * width : (index + 1) * width].astype(low).astype(jnp.float32)
        ref[:, :width] = feature_map(value).astype(low)
    v_ref[:, :width] = proj_ref[:, 2 * width : 3 * width].astype(low)
    forget = proj_ref[:, 4 * width : 4 * width + heads] + bias_ref[...]
    cum_ref[...] = jnp.zeros_like(cum_ref)
    cum_ref[:, :heads] = decay_sums(forget, length)
    cum_t_ref[...] = jnp.transpose(cum_ref[...])
    n_ref[:, :width] = attended_ref[...]

    def roots_of(value, masks):
        square = value * value
        roots = [
            lax.rsqrt(
                jnp.sum(jnp.where(mask, square, 0.0), axis=1, keepdims=True) / head_size
                + head_epsilon
            )
            for mask in masks
        ]
        return jnp.where(masks[0], roots[0], jnp.where(masks[1], roots[1], 1.0))

    def normalise(pair, _):
        window = pl.ds(pl.multiple_of(pair * 128, 128), 256)
        masks = head_masks(pair, head_size, 256)
        value = n_ref[:, window]
        root = roots_of(value, masks)
        n_ref[:, window] = value * root
        u_ref[:, window] += jnp.where(masks[0] | masks[1], root, 0.0)
        return 0

    lax.fori_loop(0, heads // 2, normalise, 0)
    gate = proj_ref[:, 3 * width : 4 * width]
    sigma = jax.nn.sigmoid(gate)
    normed = n_ref[:, :width]
    gated_low = (normed * (gate * sigma)).astype(low)
    mixed_grad = mixed_grad_ref[...]
    dq_ref[:, :width] = mixed_grad

    def one_tap(tap, _):
        matrix = tap_matrix(tap, place, images, length)
        found = jnp.dot(matrix, gated_low, preferred_element_type=jnp.float32)
        taps_grad_ref[pl.ds(tap, 1), :] = jnp.sum(
            mixed_grad_ref[...] * found, axis=0, keepdims=True
        )
        scaled = (mixed_grad_ref[...] * taps_ref[pl.ds(8 - tap, 1), :]).astype(low)
        dq_ref[:, :width] += jnp.dot(matrix, scaled, preferred_element_type=jnp.float32)
        return 0

    lax.fori_loop(0, 9, one_tap, 0)
    gated_grad = dq_ref[:, :width]
    proj_grad_ref[:, 3 * width : 4 * width] = (
        gated_grad * normed * (sigma * (1.0 + gate * (1.0 - sigma)))
    ).astype(low)
    dq_ref[:, :width] = gated_grad * (gate * sigma)
    dv_ref[...] = jnp.zeros_like(dv_ref)

    def through_norm(pair, _):
        window = pl.ds(pl.multiple_of(pair * 128, 128), 256)
        masks = head_masks(pair, head_size, 256)
        value = n_ref[:, window]
        push = dq_ref[:, window]
        product = value * push
        means = [
            jnp.sum(jnp.where(mask, product, 0.0), axis=1, keepdims=True) / head_size
            for mask in masks
        ]
        mean = jnp.where(masks[0], means[0], means[1])
        result = u_ref[:, window] * (push - value * mean)
        dv_ref[:, window] += jnp.where(masks[0] | masks[1], result, 0.0)
        return 0

    lax.fori_loop(0, heads // 2, through_norm, 0)
    o_ref[...] = dv_ref[...].astype(low)
    dv_ref[...] = jnp.zeros_like(dv_ref)
    dq_ref[...] = jnp.zeros_like(dq_ref)

    def one_pair(pair, _):
        window = pl.ds(pl.multiple_of(pair * 128, 128), 256)
        masks = head_masks(pair, head_size, 256)

        def stack(value):
            zero = jnp.zeros_like(value)
            return jnp.concatenate(
                [jnp.where(masks[0], value, zero), jnp.where(masks[1], value, zero)], axis=0
            )

        query = stack(q_ref[:, window])
        push = stack(o_ref[:, window])
        scores = dot_rows(query, k_ref[:, window])
        weights = pair_weights(pair, cum_ref, cum_t_ref, place[1], place[2], length)
        pushed = dot_rows(push, v_ref[:, window]) * weights
        moved = pushed * scores
        scores_low = (scores * weights).astype(low)
        pushed_low = pushed.astype(low)
        dv_ref[:, window] += contract_rows(scores_low, push)
        found = jnp.dot(pushed_low, k_ref[:, window], preferred_element_type=jnp.float32)
        dq_ref[:, window] += by_head(masks, found[:length], found[length:])
        dk_ref[:, window] += contract_rows(pushed_low, query)
        down = lax.broadcasted_iota(jnp.int32, (length, length), 0)
        along = lax.broadcasted_iota(jnp.int32, (length, length), 1)
        upper = jnp.where(along >= down, 1.0, 0.0).astype(low)
        lane = lax.broadcasted_iota(jnp.int32, decay_ref.shape, 1)
        for which in range(2):
            part = moved[which * length : (which + 1) * length]
            high = part.astype(low)
            rest = (part - high.astype(jnp.float32)).astype(low)
            later = jnp.dot(upper, high, preferred_element_type=jnp.float32) + jnp.dot(
                upper, rest, preferred_element_type=jnp.float32
            )
            column = jnp.sum(jnp.where(along < down, later, 0.0), axis=1, keepdims=True)
            decay_ref[...] += jnp.where(lane == 2 * pair + which, column, 0.0)
        return 0

    lax.fori_loop(0, heads // 2, one_pair, 0)
    for index, ref in enumerate((dq_ref, dk_ref)):
        value = proj_ref[:, index * width : (index + 1) * width].astype(low).astype(jnp.float32)
        slope = jnp.where(value > 0, 1.0, jnp.exp(jnp.minimum(value, 0.0)))
        proj_grad_ref[:, index * width : (index + 1) * width] = (ref[:, :width] * slope).astype(low)
    proj_grad_ref[:, 2 * width : 3 * width] = dv_ref[:, :width].astype(low)
    forget_grad = decay_ref[:, :heads] * (jax.nn.sigmoid(-forget) / gate_norm)
    proj_grad_ref[:, 4 * width : 4 * width + heads] = forget_grad.astype(low)
    bias_grad_ref[...] = jnp.sum(forget_grad, axis=0, keepdims=True)


def run_mixer(heads, heights, widths, proj, bias, taps, extra=None):
    length = proj.shape[0]
    width = taps.shape[1]
    padded = (heads // 2 - 1) * 128 + 256
    vmem = pl.BlockSpec(memory_space=pltpu.VMEM)
    smem = pl.BlockSpec(memory_space=pltpu.SMEM)
    wide = pltpu.VMEM((length, padded), jnp.float32)
    thin = pltpu.VMEM((length, padded), jnp.bfloat16)
    sums = [pltpu.VMEM((length, 128), jnp.float32), pltpu.VMEM((128, length), jnp.float32)]
    bias = bias.reshape(1, heads)
    taps = taps.astype(jnp.float32)
    if extra is None:
        return pl.pallas_call(
            functools.partial(mixer_forward, heads),
            out_shape=(
                jax.ShapeDtypeStruct((length, width), jnp.bfloat16),
                jax.ShapeDtypeStruct((length, width), jnp.float32),
            ),
            in_specs=[smem, smem, vmem, vmem, vmem],
            out_specs=(vmem, vmem),
            scratch_shapes=[thin, thin, thin, wide] + sums,
            cost_estimate=pl.CostEstimate(
                flops=10**10, bytes_accessed=4 * 10**6, transcendentals=10**6
            ),
            name="mixer_forward",
        )(heights, widths, proj, bias, taps)
    return pl.pallas_call(
        functools.partial(mixer_backward, heads),
        out_shape=(
            jax.ShapeDtypeStruct((length, proj.shape[1]), jnp.bfloat16),
            jax.ShapeDtypeStruct((9, width), jnp.float32),
            jax.ShapeDtypeStruct((1, heads), jnp.float32),
        ),
        in_specs=[smem, smem, vmem, vmem, vmem, vmem, vmem],
        out_specs=(vmem, vmem, vmem),
        scratch_shapes=[thin] * 4 + [wide] * 5 + sums + [pltpu.VMEM((length, 128), jnp.float32)],
        cost_estimate=pl.CostEstimate(
            flops=3 * 10**10, bytes_accessed=6 * 10**6, transcendentals=10**6
        ),
        name="mixer_backward",
    )(heights, widths, proj, bias, taps, *extra)


def body(
    hidden_in,
    condition,
    heights,
    widths,
    ada_weight,
    attn_weight,
    forget_weight,
    forget_bias,
    conv_weight,
    out_weight,
    up_weight,
    down_weight,
    cotangent,
    ranks=1,
):
    low = jnp.bfloat16
    sequence_count, number_of_images = heights.shape
    number_of_tokens, hidden_width = hidden_in.shape
    length = number_of_tokens // sequence_count
    half_width = conv_weight.shape[1]
    images_here = condition.shape[0]
    rows = up_weight.shape[0]
    me = lax.axis_index("dp")
    side = lax.axis_index("tensor")
    ends = jnp.cumsum(heights * widths, axis=1)
    slots = jnp.arange(length, dtype=jnp.int32)[None, :, None]
    inside = (slots < ends[:, None, :]) & (slots >= (ends - heights * widths)[:, None, :])
    choose_rows = inside.astype(jnp.float32)

    owners = np.repeat(np.array(relative_owners(ranks), np.int32), rows)
    natural = (me ^ owners) * rows + np.tile(np.arange(rows, dtype=np.int32), ranks)
    order = (jnp.arange(hidden_width, dtype=jnp.int32)[:, None] == natural[None, :]).astype(low)

    def to_relative(value):
        return jnp.dot(value, order, preferred_element_type=jnp.float32)

    def to_natural(value):
        return dot_rows(value, order)

    head_count = forget_weight.shape[1]
    proj_width = 4 * half_width + head_count
    shard_attn = jnp.concatenate([attn_weight.reshape(rows, 4 * half_width), forget_weight], axis=1)
    full_attn = gather_pieces(shard_attn, ranks, True).reshape(hidden_width, proj_width)

    cond_all = gather_pieces(condition, ranks, False).reshape(ranks * images_here, hidden_width)
    cond_own = jnp.dot(cond_all, order[:, :rows], preferred_element_type=jnp.float32)
    act_own = jax.nn.silu(cond_own).astype(low)
    mod_partial = jnp.dot(act_own, ada_weight, preferred_element_type=jnp.float32)
    mod_half = scatter_sum(mod_partial.reshape(ranks, images_here, -1), ranks, jnp.float32)
    mod_other = other_side(mod_half)
    mod_first = jnp.where(side == 0, mod_half, mod_other).reshape(images_here * 3, hidden_width)
    mod_second = jnp.where(side == 0, mod_other, mod_half).reshape(images_here * 3, hidden_width)
    mod_rel = jnp.dot(
        jnp.concatenate([mod_first, mod_second], axis=0),
        order.astype(jnp.float32),
        precision=highest_precision,
    ).reshape(2, sequence_count, number_of_images, 3, hidden_width)

    token_wise = jnp.einsum(
        "jyq,hjqcu->hcjyu", choose_rows, mod_rel, precision=highest_precision
    ).reshape(6, number_of_tokens, hidden_width)
    shift_one, scale_one, gate_one, shift_two, scale_two, gate_two = (
        token_wise[0],
        token_wise[1],
        token_wise[2],
        token_wise[3],
        token_wise[4],
        token_wise[5],
    )
    full_out = gather_pieces(out_weight.T, ranks, True).reshape(hidden_width, half_width)
    full_up = gather_pieces(up_weight, ranks, True).reshape(hidden_width, -1)
    full_down = gather_pieces(down_weight.T, ranks, True).reshape(hidden_width, -1)

    hidden_float = to_relative(hidden_in)
    upstream = to_relative(cotangent)
    modulated_one, norm_one_back = jax.vjp(modulate, hidden_float, shift_one, scale_one)
    xm_one = modulated_one.astype(low)
    projected = jnp.dot(xm_one, full_attn, preferred_element_type=jnp.float32)
    mixer = functools.partial(
        run_mixer, head_count, heights, widths, projected, forget_bias, conv_weight
    )
    mixed_low, attended = mixer()
    attn_out = tensor_total(dot_rows(mixed_low, full_out))
    after_attn = hidden_float + gate_one * attn_out
    modulated_two, norm_two_back = jax.vjp(modulate, after_attn, shift_two, scale_two)
    xm_two = modulated_two.astype(low)
    up_value = jnp.dot(xm_two, full_up, preferred_element_type=jnp.float32)
    act_value, gelu_back = jax.vjp(gelu_tanh, up_value)
    act_ffn = act_value.astype(low)
    down_value = tensor_total(dot_rows(act_ffn, full_down))
    hidden_out = to_natural((after_attn + gate_two * down_value).astype(low)).astype(low)

    delta_down = (gate_two * upstream).astype(low)
    delta_gate_two = upstream * down_value
    delta_act = jnp.dot(delta_down, full_down, preferred_element_type=jnp.float32)
    grad_down = scatter_sum(dot_tokens(delta_down, act_ffn).reshape(ranks, rows, -1), ranks, low)
    delta_up = gelu_back(delta_act)[0].astype(low)
    grad_up = scatter_sum(dot_tokens(xm_two, delta_up).reshape(ranks, rows, -1), ranks, low)
    delta_xm_two = tensor_total(dot_rows(delta_up, full_up))
    delta_after, delta_shift_two, delta_scale_two = norm_two_back(delta_xm_two)
    delta_after = delta_after + upstream
    delta_attn = (gate_one * delta_after).astype(low)
    delta_gate_one = delta_after * attn_out
    grad_out = scatter_sum(dot_tokens(delta_attn, mixed_low).reshape(ranks, rows, -1), ranks, low)
    delta_mixed = jnp.dot(delta_attn, full_out, preferred_element_type=jnp.float32)
    delta_proj, delta_conv, delta_bias = mixer((attended, delta_mixed))
    small = jnp.concatenate(
        [delta_conv, jnp.pad(delta_bias, ((0, 0), (0, half_width - head_count)))], axis=0
    )
    small = sum_everywhere(small, ranks)
    grad_conv, grad_bias = small[:-1], small[-1, :head_count]
    grad_proj = scatter_sum(dot_tokens(xm_one, delta_proj).reshape(ranks, rows, -1), ranks, low)
    delta_xm_one = tensor_total(dot_rows(delta_proj, full_attn))
    delta_input, delta_shift_one, delta_scale_one = norm_one_back(delta_xm_one)
    grad_hidden = to_natural((delta_after + delta_input).astype(low)).astype(low)
    first_group = jnp.stack([delta_shift_one, delta_scale_one, delta_gate_one], axis=0)
    second_group = jnp.stack([delta_shift_two, delta_scale_two, delta_gate_two], axis=0)
    delta_tokens = jnp.where(side == 0, first_group, second_group)
    delta_mod = jnp.einsum(
        "mxz,cmxk->mzck",
        choose_rows,
        delta_tokens.reshape(3, sequence_count, length, hidden_width),
        precision=highest_precision,
    ).reshape(images_here * 3, hidden_width)
    delta_mod = to_natural(delta_mod.astype(low)).astype(low).reshape(images_here, -1)
    delta_all = gather_pieces(delta_mod, ranks, False).reshape(ranks * images_here, -1)
    grad_ada = lax.dot_general(
        act_own, delta_all, (((0,), (0,)), ((), ())), preferred_element_type=jnp.float32
    )
    delta_cond = dot_rows(delta_all, ada_weight)
    delta_cond = delta_cond + other_side(delta_cond)
    delta_cond = exchange_pieces(delta_cond.reshape(ranks, images_here, rows), ranks)
    delta_cond = jnp.transpose(delta_cond, (1, 0, 2)).reshape(images_here, hidden_width)
    delta_cond = lax.dot_general(
        delta_cond,
        order.astype(jnp.float32),
        (((1,), (1,)), ((), ())),
        precision=highest_precision,
    )
    _, silu_back = jax.vjp(jax.nn.silu, condition.astype(jnp.float32))
    grad_condition = silu_back(delta_cond)[0].astype(low)
    return (
        hidden_out,
        grad_hidden,
        grad_condition,
        grad_ada,
        grad_proj[:, : 4 * half_width].reshape(rows, 4, half_width),
        grad_proj[:, 4 * half_width :],
        grad_bias,
        grad_conv,
        grad_out.T,
        grad_up,
        grad_down.T,
    )


def solution(mesh):
    in_specs = (
        P("dp", None),
        P("dp", None),
        P("dp", None),
        P("dp", None),
        P("dp", "tensor"),
        P("dp", None, "tensor"),
        P("dp", "tensor"),
        P("tensor"),
        P(None, "tensor"),
        P("tensor", "dp"),
        P("dp", "tensor"),
        P("tensor", "dp"),
        P("dp", None),
    )
    out_specs = (
        P("dp", None),
        P("dp", None),
        P("dp", None),
        P("dp", "tensor"),
        P("dp", None, "tensor"),
        P("dp", "tensor"),
        P("tensor"),
        P(None, "tensor"),
        P("tensor", "dp"),
        P("dp", "tensor"),
        P("tensor", "dp"),
    )
    return jax.shard_map(functools.partial(body, ranks=mesh.shape["dp"]), mesh=mesh, in_specs=in_specs, out_specs=out_specs, check_vma=False)
```
